32 devices in a mesh: dp: 2 (over core), expert: 16 (over z, y, x).
Axes of the slice: x: 2, y: 2, z: 4, core: 2. Of those that a mesh axis runs over, the one named last changes fastest.
Arguments:
- tokens: bfloat16 [4096, 3584], P(('dp', 'expert')), may hold values from -6 to 6
- cotangent: bfloat16 [4096, 3584], P(('dp', 'expert')), may hold values from -6 to 6
- gates: float32 [4096, 1], P(('dp', 'expert')), may hold values from 0.1 to 1
- routes: int32 [4096, 1], P(('dp', 'expert')), may hold values from 0 to 15; in each aligned block of 128 rows (0 to 127, 128 to 255, ...) at most 10 rows name the same one
- w_up: bfloat16 [16, 3584, 1024], P('expert', None, 'dp'), may hold values from -0.09375 to 0.09375
- w_down: bfloat16 [16, 1024, 3584], P('expert', 'dp'), may hold values from -0.1875 to 0.1875
- m_up: bfloat16 [16, 3584, 1024], P('expert', None, 'dp'), may hold values from -3 to 3
- v_up: bfloat16 [16, 3584, 1024], P('expert', None, 'dp'), may hold values from 0.099609375 to 1
- m_down: bfloat16 [16, 1024, 3584], P('expert', 'dp'), may hold values from -3 to 3
- v_down: bfloat16 [16, 1024, 3584], P('expert', 'dp'), may hold values from 0.099609375 to 1
- leaving: int32 [1], replicated, may hold values from 0 to 15
- tile_owner: int32 [16], replicated, may hold values from 0 to 15, each once
Outputs:
- update_up: bfloat16 [16, 3584, 1024], P('expert', None, 'dp')
- update_down: bfloat16 [16, 1024, 3584], P('expert', 'dp')
- adopted_up: bfloat16 [16, 224, 1024], P('expert', None, 'dp')
- adopted_down: bfloat16 [16, 224, 1024], P('expert', None, 'dp')
The draws below stay inside these ranges and needn't reach their ends.
Inputs may be any that keep to these rules, and one draw needn't show every extreme that they name: `routes`: each row names one expert; within the 128 rows of one device no expert is named more than 10 times, a bound that some block reaches in some devices. `tile_owner`: A permutation of the 16 device indices of the expert axis.
All inputs are finite; a program needn't handle non-finite values.
Results may differ from the reference program's by a relative error of at most 0.0041.
Values may be sent and summed in bfloat16 or wider, within the bound.
A program may use at most 128 MiB of HBM per device.

```python
import math
import jax
import jax.numpy as jnp
import numpy as np
from jax import lax

D = 3584
FF = 1024
TOK_DEV = 128
TOPK = 1
EXPERTS = 16
TOKENS = 4096
CAP = 10
DEVICES = 32


def level_of(key, shape, shards, smallest, largest):
    factor_of, own = 1.0, jax.random.fold_in(key, 6)
    for position, shards_of in shards:
        heights = jnp.exp(jax.random.uniform(jax.random.fold_in(own, position), (shards_of,), jnp.float32, smallest / len(shards), largest / len(shards)))
        factor_of = factor_of * jnp.repeat(heights, shape[position] // shards_of).reshape([-1 if axis == position else 1 for axis in range(len(shape))])
    return factor_of


def deal_out(stream_key, own, number, rows, count, top, reach, skew):
    order = jax.random.permutation(stream_key, count)
    packed, ordinary = portions_of(count, rows * top, reach, skew, True), portions_of(count, rows * top, reach, skew, False)
    places = jnp.arange(count)

    def named(sizes, rotation):
        used = int((sizes > 0).sum())
        fixed = max(1, used // 4)
        shifted = fixed + (places - fixed + rotation * (used - fixed)) % max(1, count - fixed)
        return jnp.zeros((count,), jnp.int32).at[order[jnp.where(places < fixed, places, shifted)]].set(jnp.asarray(sizes, jnp.int32))

    sizes = jnp.where(number % 4 == 0, named(packed, number // 4), named(ordinary, number - number // 4 - 1))
    mixed = jax.random.permutation(jax.random.fold_in(own, 3), count)
    giver, receiver = mixed[0:count // 2 * 2:2], mixed[1:count // 2 * 2:2]
    room = jnp.minimum(sizes[giver] - 1, reach - sizes[receiver]) // 2
    room = jnp.where((giver == order[0]) | (receiver == order[0]) | (sizes[receiver] == 0), 0, jnp.maximum(room, 0))
    shifted = jax.random.randint(jax.random.fold_in(own, 4), (count // 2,), 0, 1 << 20) % (room + 1)
    sizes = sizes.at[giver].add(-shifted).at[receiver].add(shifted)
    labels = jnp.searchsorted(jnp.cumsum(sizes), jnp.arange(rows * top), side="right").astype(jnp.int32)
    listing = labels.reshape(top, rows).T
    listing = listing[jax.random.permutation(jax.random.fold_in(own, 1), rows)]
    rotation = jax.random.randint(jax.random.fold_in(own, 2), (rows, 1), 0, top)
    return jnp.take_along_axis(listing, (jnp.arange(top)[None, :] + rotation) % top, axis=1)


def portions_of(number_of, total, bound, lean, full):
    weights = [(1 << 20) // math.isqrt(grade ** lean) + 1 for grade in range(1, number_of + 1)]
    largest = bound if full else min(bound, max(-(-total // number_of), total * weights[0] // sum(weights)))
    least = 1 if total - largest >= number_of - 1 else 0
    holding, rest = [largest] + [least] * (number_of - 1), total - largest - least * (number_of - 1)
    while rest > 0:
        candidates = [i for i in range(1, number_of) if holding[i] < largest] or [i for i in range(1, number_of) if holding[i] < bound]
        whole, remaining = sum([weights[i] for i in candidates]), rest
        for i in candidates:
            addition = min(bound - holding[i], max(1, remaining * weights[i] // whole), rest)
            holding[i] = holding[i] + addition
            rest = rest - addition
    return np.array(holding)


def centred(key, dims, spread, limit, split=(), kind=jnp.bfloat16):
    drawn = jax.random.normal(key, dims, jnp.float32) * spread
    if len(split) > 0:
        drawn = level_of(key, dims, split, -0.22, 0.18) * drawn
    return jnp.clip(drawn, min=-limit, max=limit).astype(kind)


def setup_inputs(seed: int = 0) -> dict:
    streams_of = jax.random.split(jax.random.key(seed), 13)
    tokens = centred(streams_of[0], (TOKENS, D), 1.0, 6.0, ((0, 32),))
    cotangent = centred(streams_of[1], (TOKENS, D), 1.0, 6.0, ((0, 32),))
    gates = jnp.clip(jnp.exp(math.log(1.0) - 2.3025851 * jax.random.uniform(streams_of[2], (TOKENS, TOPK), jnp.float32) ** level_of(streams_of[2], (TOKENS, TOPK), ((0, 32),), -0.2, 0.2)), 0.1, 1.0)
    routes_keys = jax.random.split(jax.random.fold_in(streams_of[3], 1), TOKENS // TOK_DEV)
    routes_turns = jax.random.permutation(jax.random.fold_in(streams_of[3], 3), TOKENS // TOK_DEV)
    routes = jax.vmap(lambda own, number: deal_out(jax.random.fold_in(streams_of[3], 2), own, number, TOK_DEV, EXPERTS, TOPK, CAP, 1))(routes_keys, routes_turns).reshape((TOKENS, TOPK))
    w_up = centred(streams_of[4], (EXPERTS, D, FF), D ** -0.5, 0.09375, ((0, 16), (2, 2)))
    w_down = centred(streams_of[5], (EXPERTS, FF, D), FF ** -0.5, 0.1875, ((0, 16), (1, 2)))
    m_up = centred(streams_of[6], (EXPERTS, D, FF), 0.5, 3.0, ((0, 16), (2, 2)))
    v_up = jnp.clip(jnp.exp(math.log(1.0) - 2.306499 * jax.random.uniform(streams_of[7], (EXPERTS, D, FF), jnp.float32) ** level_of(streams_of[7], (EXPERTS, D, FF), ((0, 16), (2, 2)), -0.2, 0.2)), 0.099609375, 1.0).astype(jnp.bfloat16)
    m_down = centred(streams_of[8], (EXPERTS, FF, D), 0.5, 3.0, ((0, 16), (1, 2)))
    v_down = jnp.clip(jnp.exp(math.log(1.0) - 2.306499 * jax.random.uniform(streams_of[9], (EXPERTS, FF, D), jnp.float32) ** level_of(streams_of[9], (EXPERTS, FF, D), ((0, 16), (1, 2)), -0.2, 0.2)), 0.099609375, 1.0).astype(jnp.bfloat16)
    leaving = jax.random.randint(streams_of[10], (1,), 0, EXPERTS).astype(jnp.int32)
    tile_owner = jax.random.permutation(streams_of[11], EXPERTS).astype(jnp.int32)
    return {"tokens": tokens, "cotangent": cotangent, "gates": gates, "routes": routes, "w_up": w_up, "w_down": w_down, "m_up": m_up, "v_up": v_up, "m_down": m_down, "v_down": v_down, "leaving": leaving, "tile_owner": tile_owner}


BETA_ONE = 0.9
BETA_TWO = 0.95
EPSILON = 1e-08

def expert_terms(rows_x, rows_c, up_tile, down_tile):
    preact = jnp.dot(rows_x, up_tile, preferred_element_type=jnp.float32)
    squash = jax.nn.sigmoid(preact)
    hidden = (preact * squash).astype(jnp.bfloat16)
    slope_val = squash * (1.0 + preact * (1.0 - squash))
    back_grad = lax.dot_general(rows_c, down_tile, (((1,), (1,)), ((), ())), preferred_element_type=jnp.float32)
    pre_grad = (back_grad * slope_val).astype(jnp.bfloat16)
    grad_up = lax.dot_general(rows_x, pre_grad, (((0,), (0,)), ((), ())), preferred_element_type=jnp.float32)
    grad_cols = lax.dot_general(rows_c, hidden, (((0,), (0,)), ((), ())), preferred_element_type=jnp.float32)
    return (grad_up, grad_cols)

def adam_step(gradient, moment_one, moment_two):
    new_one = BETA_ONE * moment_one.astype(jnp.float32) + (1.0 - BETA_ONE) * gradient
    new_two = BETA_TWO * moment_two.astype(jnp.float32) + (1.0 - BETA_TWO) * gradient * gradient
    return (new_one / (jnp.sqrt(new_two) + EPSILON)).astype(jnp.bfloat16)

def reference(tokens, cotangent, gates, routes, w_up, w_down, m_up, v_up, m_down, v_down, leaving, tile_owner):
    experts = w_up.shape[0]
    hidden_units = w_up.shape[2]
    tok_count, model_width = tokens.shape
    top_count = routes.shape[1]
    pair_count = tok_count * top_count
    expert_of = routes.reshape(pair_count)
    pair_x = jnp.repeat(tokens, top_count, axis=0)
    pair_c = (gates.reshape(pair_count)[:, None] * jnp.repeat(cotangent, top_count, axis=0).astype(jnp.float32)).astype(jnp.bfloat16)
    most_rows = DEVICES * CAP

    def one_expert(expert_id):
        sort_key = jnp.where(expert_of == expert_id, 0, 1).astype(jnp.int32)
        row_order = jnp.argsort(sort_key, stable=True)[:most_rows]
        is_valid = (expert_of[row_order] == expert_id)[:, None]
        rows_x = jnp.where(is_valid, pair_x[row_order], jnp.zeros((), jnp.bfloat16))
        rows_c = jnp.where(is_valid, pair_c[row_order], jnp.zeros((), jnp.bfloat16))
        up_tile = lax.dynamic_index_in_dim(w_up, expert_id, 0, keepdims=False)
        down_tile = lax.dynamic_index_in_dim(w_down, expert_id, 0, keepdims=False)
        grad_up, grad_cols = expert_terms(rows_x, rows_c, up_tile, down_tile)
        step_up = adam_step(grad_up, lax.dynamic_index_in_dim(m_up, expert_id, 0, keepdims=False), lax.dynamic_index_in_dim(v_up, expert_id, 0, keepdims=False))
        step_down = adam_step(grad_cols.T, lax.dynamic_index_in_dim(m_down, expert_id, 0, keepdims=False), lax.dynamic_index_in_dim(v_down, expert_id, 0, keepdims=False))
        return (step_up, step_down)
    expert_ids = jnp.arange(experts, dtype=jnp.int32)
    steps_up, steps_down = lax.map(one_expert, expert_ids)
    leaver = leaving[0]
    keep_own = (expert_ids != leaver)[:, None, None]
    update_up = jnp.where(keep_own, steps_up, jnp.zeros((), jnp.bfloat16))
    update_down = jnp.where(keep_own, steps_down, jnp.zeros((), jnp.bfloat16))
    leaver_up = lax.dynamic_index_in_dim(steps_up, leaver, 0, keepdims=False)
    leaver_down = lax.dynamic_index_in_dim(steps_down, leaver, 0, keepdims=False)
    tile_rows = model_width // experts
    adopt = lax.optimization_barrier(jnp.sum(jnp.where(tile_owner[None, :] == expert_ids[:, None], expert_ids[None, :], 0), axis=1)).astype(jnp.int32)
    adopted_up = leaver_up.reshape(experts, tile_rows, hidden_units)[adopt]
    adopted_down = leaver_down.T.reshape(experts, tile_rows, hidden_units)[adopt]
    return (update_up, update_down, adopted_up, adopted_down)
```

```python
import functools

import jax
import jax.numpy as jnp
from jax import lax
from jax.experimental import pallas as pl
from jax.experimental.pallas import tpu as pltpu
from jax.sharding import PartitionSpec as P

BETA_ONE = 0.9
BETA_TWO = 0.95
EPSILON = 1e-08
MESH = pl.DeviceIdType.MESH


def expert_terms(rows_x, rows_c, up_tile, down_tile):
    preact = jnp.dot(rows_x, up_tile, preferred_element_type=jnp.float32)
    squash = jax.nn.sigmoid(preact)
    hidden = (preact * squash).astype(jnp.bfloat16)
    slope_val = squash * (1.0 + preact * (1.0 - squash))
    back_grad = lax.dot_general(
        rows_c, down_tile, (((1,), (1,)), ((), ())), preferred_element_type=jnp.float32
    )
    pre_grad = (back_grad * slope_val).astype(jnp.bfloat16)
    grad_up = lax.dot_general(
        rows_x, pre_grad, (((0,), (0,)), ((), ())), preferred_element_type=jnp.float32
    )
    grad_cols = lax.dot_general(
        rows_c, hidden, (((0,), (0,)), ((), ())), preferred_element_type=jnp.float32
    )
    return (grad_up, grad_cols)


def adam_step(gradient, moment_one, moment_two):
    new_one = BETA_ONE * moment_one.astype(jnp.float32) + (1.0 - BETA_ONE) * gradient
    new_two = BETA_TWO * moment_two.astype(jnp.float32) + (1.0 - BETA_TWO) * gradient * gradient
    return (new_one / (jnp.sqrt(new_two) + EPSILON)).astype(jnp.bfloat16)


def on_device(
    tokens, cotangent, gates, routes, w_up, w_down, m_up, v_up, m_down, v_down, leaving, tile_owner
):
    experts = lax.axis_size("expert")
    my_index = lax.axis_index("expert")
    tok_count, model_width = tokens.shape
    top_count = routes.shape[1]
    hidden_units = w_up.shape[2]
    capacity = 5 * tok_count * top_count // (4 * experts)
    pair_count = tok_count * top_count
    leaver = leaving[0]
    slot_ids = jnp.arange(experts, dtype=jnp.int32)
    tile_rows = model_width // experts
    adopt = jnp.sum(
        jnp.where(tile_owner[None, :] == slot_ids[:, None], slot_ids[None, :], 0), axis=1
    )
    expert_of = routes.reshape(pair_count)
    member = (expert_of[:, None] == slot_ids[None, :]).astype(jnp.int32)
    slot_rank = jnp.sum((jnp.cumsum(member, axis=0) - 1) * member, axis=1)
    slot_place = expert_of * capacity + slot_rank
    staying = expert_of != leaver
    send_mask = jnp.ones_like(staying)
    pair_x = jnp.repeat(tokens, top_count, axis=0)
    pair_c = (
        gates.reshape(pair_count)[:, None]
        * jnp.repeat(cotangent, top_count, axis=0).astype(jnp.float32)
    ).astype(jnp.bfloat16)
    pair_both = jnp.concatenate([pair_x, pair_c], axis=1)
    targets = jnp.arange(experts * capacity, dtype=jnp.int32)
    picker = ((slot_place[None, :] == targets[:, None]) & send_mask[None, :]).astype(jnp.bfloat16)
    send_both = jnp.dot(picker, pair_both, preferred_element_type=jnp.float32).astype(jnp.bfloat16)
    send_x = send_both[:, :model_width].reshape(experts, capacity, model_width)
    send_c = send_both[:, model_width:].reshape(experts, capacity, model_width)
    recv_x, recv_c = (
        lax.all_to_all(send_x, "expert", split_axis=0, concat_axis=0, tiled=True),
        lax.all_to_all(send_c, "expert", split_axis=0, concat_axis=0, tiled=True),
    )
    recv_x = recv_x.reshape(experts * capacity, model_width)
    recv_c = recv_c.reshape(experts * capacity, model_width)
    grad_up, grad_cols = expert_terms(
        lax.all_gather(recv_x, "dp", axis=0, tiled=True),
        lax.all_gather(recv_c, "dp", axis=0, tiled=True),
        w_up[0],
        w_down[0],
    )
    keep_own = my_index != leaver
    step_up = adam_step(grad_up, m_up[0], v_up[0])
    step_down = adam_step(grad_cols.T, m_down[0], v_down[0])
    both_steps = jnp.concatenate([step_up, step_down.T], axis=1).reshape(
        experts, tile_rows, 2 * hidden_units
    )
    ordered = both_steps[adopt]
    outgoing = jnp.where(keep_own, jnp.zeros_like(ordered), ordered)
    incoming = lax.all_to_all(outgoing, "expert", split_axis=0, concat_axis=0, tiled=True)
    mine = lax.dynamic_index_in_dim(incoming, leaver, 0, keepdims=False)
    adopted_up = mine[:, :hidden_units][None]
    adopted_down = mine[:, hidden_units:][None]
    update_up = jnp.where(keep_own, step_up, jnp.zeros_like(step_up))[None]
    update_down = jnp.where(keep_own, step_down, jnp.zeros_like(step_down))[None]
    return (update_up, update_down, adopted_up, adopted_down)


def round_up(value, step):
    return -(-value // step) * step


def dispatch_kernel(
    experts, replicas, cap, slot,
    routes_ref, gates_ref, tok_ref, cot_ref, w_up_hbm, w_down_hbm,
    rows_hbm, hidden_hbm, pre_hbm,
    send, recv, full, w_up, w_down, hidden, pre_grad,
    send_sem, recv_sem, pass_sem, land_sem, load_sem, out_sem,
):
    me = lax.axis_index("expert")
    my_rep = lax.axis_index("dp")
    tok_count, width = tok_ref.shape
    load_up = pltpu.make_async_copy(w_up_hbm, w_up, load_sem.at[0])
    load_down = pltpu.make_async_copy(w_down_hbm, w_down, load_sem.at[1])
    load_up.start()
    load_down.start()

    barrier = pltpu.get_barrier_semaphore()

    def zero(step, carry):
        full[step] = jnp.zeros(full.shape[1:], full.dtype)
        return carry

    lax.fori_loop(0, replicas * experts, zero, 0)
    for k in range(1, experts):
        pl.semaphore_signal(
            barrier, inc=1, device_id={"expert": lax.rem(me + k, experts)}, device_id_type=MESH
        )
    for j in range(1, replicas):
        pl.semaphore_signal(
            barrier, inc=1, device_id={"dp": lax.rem(my_rep + j, replicas)}, device_id_type=MESH
        )

    names = lax.broadcasted_iota(jnp.int32, (tok_count, experts), 1)
    member = routes_ref[...] == names
    before = (
        lax.broadcasted_iota(jnp.int32, (tok_count, tok_count), 0)
        > lax.broadcasted_iota(jnp.int32, (tok_count, tok_count), 1)
    )
    member_f = member.astype(jnp.float32)
    rank = jnp.dot(
        before.astype(jnp.float32).astype(jnp.bfloat16),
        member_f.astype(jnp.bfloat16),
        preferred_element_type=jnp.float32,
    )
    place = jnp.sum(
        member_f * (rank + (names * slot).astype(jnp.float32)), axis=1, keepdims=True
    )
    spots = lax.broadcasted_iota(jnp.int32, (tok_count, experts * slot), 1).astype(jnp.float32)
    picker = (place == spots).astype(jnp.float32).astype(jnp.bfloat16)
    part = width // 4
    for j in range(4):
        block = tok_ref[:, j * part : (j + 1) * part]
        picked = lax.dot_general(
            picker, block, (((0,), (0,)), ((), ())), preferred_element_type=jnp.float32
        ).astype(jnp.bfloat16)
        send[:, :, j * part : (j + 1) * part] = picked.reshape(experts, slot, part)[:, :cap]
        block = (
            gates_ref[...] * cot_ref[:, j * part : (j + 1) * part].astype(jnp.float32)
        ).astype(jnp.bfloat16)
        picked = lax.dot_general(
            picker, block, (((0,), (0,)), ((), ())), preferred_element_type=jnp.float32
        ).astype(jnp.bfloat16)
        send[:, :, width + j * part : width + (j + 1) * part] = picked.reshape(
            experts, slot, part
        )[:, :cap]

    pl.semaphore_wait(barrier, experts - 1 + replicas - 1)

    mine = my_rep * experts

    def post(k):
        dest = lax.rem(me + k, experts)
        return pltpu.make_async_remote_copy(
            src_ref=send.at[dest],
            dst_ref=recv.at[mine + me],
            send_sem=send_sem.at[k],
            recv_sem=recv_sem.at[k],
            device_id={"expert": dest},
            device_id_type=MESH,
        )

    def share(k, j, source):
        return pltpu.make_async_remote_copy(
            src_ref=source,
            dst_ref=recv.at[mine + lax.rem(me + experts - k, experts)],
            send_sem=pass_sem.at[j, k],
            recv_sem=land_sem.at[j, k],
            device_id={"dp": lax.rem(my_rep + j, replicas)},
            device_id_type=MESH,
        )

    def start_post(k, carry):
        post(k).start()
        return carry

    lax.fori_loop(1, experts, start_post, 0)
    for j in range(1, replicas):
        share(0, j, send.at[me]).start()
    full[mine + me, :cap, :] = send[me]

    def pass_on(k, carry):
        post(k).wait_recv()
        for j in range(1, replicas):
            share(
                k, j, recv.at[mine + lax.rem(me + experts - k, experts)]
            ).start()
        here = mine + lax.rem(me + experts - k, experts)
        full[here, :cap, :] = recv[here]
        return carry

    lax.fori_loop(1, experts, pass_on, 0)
    load_up.wait()
    load_down.wait()

    def settle(k, carry):
        for j in range(1, replicas):
            share(k, j, send.at[me]).wait_recv()
            there = lax.rem(my_rep + replicas - j, replicas) * experts
            there = there + lax.rem(me + experts - k, experts)
            full[there, :cap, :] = recv[there]
        return carry

    lax.fori_loop(0, experts, settle, 0)
    row_copy = pltpu.make_async_copy(full, rows_hbm, out_sem.at[0])
    row_copy.start()

    rows = replicas * experts * slot
    groups = 4 if (replicas * experts) % 4 == 0 else 1
    span = replicas * experts // groups

    def forward(g, carry):
        base = g * span
        preact = jnp.dot(
            full[pl.ds(base, span), :, :width].reshape(span * slot, width),
            w_up[...],
            preferred_element_type=jnp.float32,
        )
        squash = jax.nn.sigmoid(preact)
        back = lax.dot_general(
            full[pl.ds(base, span), :, width:].reshape(span * slot, width),
            w_down[...],
            (((1,), (1,)), ((), ())),
            preferred_element_type=jnp.float32,
        )
        at = pl.ds(pl.multiple_of(g * (span * slot), 16), span * slot)
        hidden[at, :] = (preact * squash).astype(jnp.bfloat16)
        pre_grad[at, :] = (back * (squash * (1.0 + preact * (1.0 - squash)))).astype(jnp.bfloat16)
        return carry

    lax.fori_loop(0, groups, forward, 0)
    hidden_copy = pltpu.make_async_copy(hidden, hidden_hbm, out_sem.at[1])
    pre_copy = pltpu.make_async_copy(pre_grad, pre_hbm, out_sem.at[2])
    hidden_copy.start()
    pre_copy.start()

    def finish(k, carry):
        for j in range(1, replicas):
            share(k, j, send.at[me]).wait_send()
        return carry

    def finish_post(k, carry):
        post(k).wait_send()
        return carry

    lax.fori_loop(1, experts, finish_post, 0)
    lax.fori_loop(0, experts, finish, 0)
    row_copy.wait()
    hidden_copy.wait()
    pre_copy.wait()


def dispatch(tokens, cotangent, gates, routes, up_tile, down_tile, experts, replicas, cap, slot):
    width = tokens.shape[1]
    units = up_tile.shape[1]
    rows = replicas * experts * slot
    vmem = pl.BlockSpec(memory_space=pltpu.VMEM)
    hbm = pl.BlockSpec(memory_space=pl.ANY)
    return pl.pallas_call(
        functools.partial(dispatch_kernel, experts, replicas, cap, slot),
        out_shape=(
            jax.ShapeDtypeStruct((replicas * experts, slot, 2 * width), jnp.bfloat16),
            jax.ShapeDtypeStruct((rows, units), jnp.bfloat16),
            jax.ShapeDtypeStruct((rows, units), jnp.bfloat16),
        ),
        in_specs=[vmem, vmem, vmem, vmem, hbm, hbm],
        out_specs=[hbm, hbm, hbm],
        scratch_shapes=[
            pltpu.VMEM((experts, cap, 2 * width), jnp.bfloat16),
            pltpu.VMEM((replicas * experts, cap, 2 * width), jnp.bfloat16),
            pltpu.VMEM((replicas * experts, slot, 2 * width), jnp.bfloat16),
            pltpu.VMEM(up_tile.shape, jnp.bfloat16),
            pltpu.VMEM(down_tile.shape, jnp.bfloat16),
            pltpu.VMEM((rows, units), jnp.bfloat16),
            pltpu.VMEM((rows, units), jnp.bfloat16),
            pltpu.SemaphoreType.DMA((experts,)),
            pltpu.SemaphoreType.DMA((experts,)),
            pltpu.SemaphoreType.DMA((replicas, experts)),
            pltpu.SemaphoreType.DMA((replicas, experts)),
            pltpu.SemaphoreType.DMA((2,)),
            pltpu.SemaphoreType.DMA((3,)),
        ],
        compiler_params=pltpu.CompilerParams(
            collective_id=0, has_side_effects=True, vmem_limit_bytes=60 * 2**20
        ),
        name="dispatch",
    )(routes, gates, tokens, cotangent, up_tile, down_tile)


def step_kernel(
    tile_rows, leaves_ref, owner_ref,
    x_ref, c_ref, hidden_ref, pre_ref, m_up, v_up, m_down, v_down,
    out_up, out_down, tiles_up, tiles_down,
):
    leaves = leaves_ref[0] == 1
    span, units = out_up.shape
    first = pl.program_id(0) * (span // tile_rows)

    for at in range(0, span, 128):
        grad = lax.dot_general(
            x_ref[:, at : at + 128], pre_ref[...], (((0,), (0,)), ((), ())),
            preferred_element_type=jnp.float32,
        )
        out_up[at : at + 128, :] = adam_fast(grad, m_up[at : at + 128, :], v_up[at : at + 128, :])
    for at in range(0, units, 128):
        grad = lax.dot_general(
            hidden_ref[:, at : at + 128], c_ref[...], (((0,), (0,)), ((), ())),
            preferred_element_type=jnp.float32,
        )
        out_down[at : at + 128, :] = adam_fast(
            grad, m_down[at : at + 128, :], v_down[at : at + 128, :]
        )

    @pl.when(leaves)
    def _():
        turned = out_down[...].T
        for j in range(span // tile_rows):
            owner = owner_ref[first + j]
            tiles_up[owner] = out_up[j * tile_rows : (j + 1) * tile_rows, :]
            tiles_down[owner] = turned[j * tile_rows : (j + 1) * tile_rows, :]
        out_up[...] = jnp.zeros_like(out_up)
        out_down[...] = jnp.zeros_like(out_down)


def adam_fast(gradient, moment_one, moment_two):
    new_one = BETA_ONE * moment_one.astype(jnp.float32) + (1.0 - BETA_ONE) * gradient
    new_two = BETA_TWO * moment_two.astype(jnp.float32) + (1.0 - BETA_TWO) * gradient * gradient
    root = jnp.sqrt(new_two) + EPSILON
    return (new_one / root).astype(jnp.bfloat16)


def grad_step(rows, hidden, pre_grad, m_up, v_up, m_down, v_down, leaves, tile_owner, span, tile_rows):
    count, double = rows.shape
    width, units = m_up.shape
    steps = width // span
    tiles = width // tile_rows
    return pl.pallas_call(
        functools.partial(step_kernel, tile_rows),
        grid_spec=pltpu.PrefetchScalarGridSpec(
            num_scalar_prefetch=2,
            grid=(steps,),
            in_specs=[
                pl.BlockSpec((count, span), lambda i, *_: (0, i)),
                pl.BlockSpec((count, span), lambda i, *_: (0, i + steps)),
                pl.BlockSpec((count, units), lambda i, *_: (0, 0)),
                pl.BlockSpec((count, units), lambda i, *_: (0, 0)),
                pl.BlockSpec((span, units), lambda i, *_: (i, 0)),
                pl.BlockSpec((span, units), lambda i, *_: (i, 0)),
                pl.BlockSpec((units, span), lambda i, *_: (0, i)),
                pl.BlockSpec((units, span), lambda i, *_: (0, i)),
            ],
            out_specs=[
                pl.BlockSpec((span, units), lambda i, *_: (i, 0)),
                pl.BlockSpec((units, span), lambda i, *_: (0, i)),
                pl.BlockSpec((tiles, tile_rows, units), lambda i, *_: (0, 0, 0)),
                pl.BlockSpec((tiles, tile_rows, units), lambda i, *_: (0, 0, 0)),
            ],
        ),
        out_shape=(
            jax.ShapeDtypeStruct((width, units), jnp.bfloat16),
            jax.ShapeDtypeStruct((units, width), jnp.bfloat16),
            jax.ShapeDtypeStruct((tiles, tile_rows, units), jnp.bfloat16),
            jax.ShapeDtypeStruct((tiles, tile_rows, units), jnp.bfloat16),
        ),
        compiler_params=pltpu.CompilerParams(vmem_limit_bytes=60 * 2**20),
        name="grad_step",
    )(leaves, tile_owner, rows, rows, hidden, pre_grad, m_up, v_up, m_down, v_down)


def scatter_kernel(leaver, experts, up_src, down_src, up_dst, down_dst, send_sem, recv_sem, own_sem):
    me = lax.axis_index("expert")

    def copies(d):
        return [
            pltpu.make_async_remote_copy(
                src_ref=src.at[d],
                dst_ref=dst,
                send_sem=send_sem.at[i, d],
                recv_sem=recv_sem.at[i],
                device_id={"expert": d},
                device_id_type=MESH,
            )
            for i, (src, dst) in enumerate(((up_src, up_dst), (down_src, down_dst)))
        ]

    @pl.when(me == leaver)
    def _():
        others = [(leaver + experts // 2 + k) % experts for k in range(experts)]
        others.remove(leaver)
        for d in others:
            for copy in copies(d):
                copy.start()
        own = [
            pltpu.make_async_copy(up_src.at[leaver], up_dst, own_sem.at[0]),
            pltpu.make_async_copy(down_src.at[leaver], down_dst, own_sem.at[1]),
        ]
        for copy in own:
            copy.start()
        for copy in own:
            copy.wait()
        for d in others:
            for copy in copies(d):
                copy.wait_send()

    @pl.when(me != leaver)
    def _():
        for copy in copies((leaver + 1) % experts):
            copy.wait_recv()


def scatter(leaver, experts, tiles_up, tiles_down):
    hbm = pl.BlockSpec(memory_space=pl.ANY)
    one = jax.ShapeDtypeStruct(tiles_up.shape[1:], jnp.bfloat16)
    return pl.pallas_call(
        functools.partial(scatter_kernel, leaver, experts),
        out_shape=(one, one),
        in_specs=[hbm, hbm],
        out_specs=[hbm, hbm],
        scratch_shapes=[
            pltpu.SemaphoreType.DMA((2, experts)),
            pltpu.SemaphoreType.DMA((2,)),
            pltpu.SemaphoreType.DMA((2,)),
        ],
        compiler_params=pltpu.CompilerParams(has_side_effects=True),
        name=f"scatter_{leaver}",
    )(tiles_up, tiles_down)


def on_device_kernels(
    tokens, cotangent, gates, routes, w_up, w_down, m_up, v_up, m_down, v_down, leaving, tile_owner
):
    experts, replicas = lax.axis_size("expert"), lax.axis_size("dp")
    width, units = w_up.shape[1:]
    cap, slot = row_bound(tokens, routes, experts)
    tile_rows = width // experts
    leaver = leaving[0]
    rows, hidden, pre_grad = dispatch(
        tokens, cotangent, gates, routes, w_up[0], w_down[0], experts, replicas, cap, slot
    )
    leaves = (lax.axis_index("expert") == leaver).astype(jnp.int32).reshape(1)
    update_up, update_down, tiles_up, tiles_down = grad_step(
        rows.reshape(-1, rows.shape[-1]), hidden, pre_grad,
        m_up[0], v_up[0], m_down[0], v_down[0], leaves, tile_owner, width // 4, tile_rows,
    )
    adopted_up, adopted_down = lax.switch(
        leaver,
        [functools.partial(scatter, e, experts) for e in range(experts)],
        tiles_up, tiles_down,
    )
    return (update_up[None], update_down[None], adopted_up[None], adopted_down[None])


def row_bound(tokens, routes, experts):
    cap = 5 * tokens.shape[0] * routes.shape[1] // (4 * experts)
    return cap, round_up(cap, 16)


def solution(mesh):
    placed = (
        P(("dp", "expert"), None),
        P(("dp", "expert"), None),
        P(("dp", "expert"), None),
        P(("dp", "expert"), None),
        P("expert", None, "dp"),
        P("expert", "dp", None),
        P("expert", None, "dp"),
        P("expert", None, "dp"),
        P("expert", "dp", None),
        P("expert", "dp", None),
        P(),
        P(),
    )
    small = mesh.shape["dp"] * mesh.shape["expert"] * 16 <= 1024
    return jax.shard_map(
        on_device_kernels if small else on_device,
        mesh=mesh,
        in_specs=placed,
        out_specs=(
            P("expert", None, "dp"),
            P("expert", "dp", None),
            P("expert", None, "dp"),
            P("expert", None, "dp"),
        ),
        check_vma=False,
    )
```
